32 devices in a mesh: blk: 16 (over z, y, core), grp: 2 (over x).
Axes of the slice: x: 2, y: 2, z: 4, core: 2. Of those that a mesh axis runs over, the one named last changes fastest.
Arguments:
- matrix_sat: float32 [512, 65536], P('grp', 'blk'), may hold values from -0.07883404 to 0.07883404
- matrix_ter: float32 [512, 65536], P('grp', 'blk'), may hold values from -0.07883404 to 0.07883404
- probes: float32 [16, 65536], P(None, 'blk'), may hold values from -6 to 6
Outputs:
- row_part: float32 [2, 16, 512], P(None, None, 'grp')
- column_part: float32 [2, 16, 65536], P(None, None, ('blk', 'grp'))
- trace_terms: float32 [2, 16], replicated
The draws below stay inside these ranges and needn't reach their ends.
All inputs are finite; a program needn't handle non-finite values.
Results may differ from the reference program's by a relative error of at most 0.000096.
Values sent between devices are 32-bit elements; how exact they have to be, the bound alone decides.
A program may use at most 64 MiB of HBM per device.

```python
import jax
import jax.numpy as jnp
from jax import lax

PROBES = 16
ORDER = 65536
SLAB = 512


def shard_levels(rng, extent, cuts, low, top_value):
    def one(dim, blocks):
        draws = jax.random.uniform(jax.random.fold_in(jax.random.fold_in(rng, 6), dim), (blocks,), jnp.float32, low / len(cuts), top_value / len(cuts))
        return jnp.repeat(jnp.exp(draws), extent[dim] // blocks).reshape((-1,) + (1,) * (len(extent) - dim - 1))

    factor_of = one(*cuts[0])
    for cut in cuts[1:]:
        factor_of = factor_of * one(*cut)
    return factor_of


def normal_values(key, shape, spread, bound, pieces=(), held_as=jnp.bfloat16):
    drawn = spread * jax.random.normal(key, shape, jnp.float32)
    if pieces:
        drawn = drawn * shard_levels(key, shape, pieces, -0.22, 0.18)
    return jnp.clip(drawn, -bound, bound).astype(held_as)


def setup_inputs(seed: int = 0) -> dict:
    splits = jax.random.split(jax.random.key(seed), 4)
    return {
        "matrix_sat": normal_values(splits[0], (SLAB, ORDER), ((SLAB * ORDER) ** -0.25), 0.07883404, ((0, 2), (1, 16)), jnp.float32),
        "matrix_ter": normal_values(splits[1], (SLAB, ORDER), ((SLAB * ORDER) ** -0.25), 0.07883404, ((0, 2), (1, 16)), jnp.float32),
        "probes": normal_values(splits[2], (PROBES, ORDER), 1.0, 6.0, ((1, 16),), jnp.float32),
    }


def one_matrix(matrix, probes):
    rows = jnp.arange(SLAB, dtype=jnp.int32)
    upper_mask = rows[None, :] >= rows[:, None]
    strict_mask = rows[None, :] > rows[:, None]
    head = matrix[:, :SLAB]
    tail = matrix[:, SLAB:]
    slab_probes = probes[:, :SLAB]
    hp = lax.Precision.HIGHEST
    direct = jnp.dot(slab_probes, jnp.where(upper_mask, head, 0.0).T, precision=hp)
    direct = direct + jnp.dot(probes[:, SLAB:], tail.T, precision=hp)
    mirror_head = jnp.dot(slab_probes, jnp.where(strict_mask, head, 0.0), precision=hp)
    mirror_tail = jnp.dot(slab_probes, tail, precision=hp)
    mirrored = jnp.concatenate([mirror_head, mirror_tail], axis=1)
    trace = jnp.sum(slab_probes * direct, axis=1) + jnp.sum(probes * mirrored, axis=1)
    return direct, mirrored, trace


def reference(matrix_sat, matrix_ter, probes):
    d_one, m_one, t_one = one_matrix(matrix_sat, probes)
    d_two, m_two, t_two = one_matrix(matrix_ter, probes)
    return jnp.stack([d_one, d_two]), jnp.stack([m_one, m_two]), jnp.stack([t_one, t_two])
```

```python
import functools

import jax
import jax.numpy as jnp
from jax import lax
from jax.experimental import pallas as pl
from jax.experimental.pallas import tpu as pltpu
from jax.sharding import PartitionSpec as P

MESH = pl.DeviceIdType.MESH
BF = jnp.bfloat16
F32 = jnp.float32


def halves(x):
    high = x.astype(BF)
    return high, (x - high.astype(F32)).astype(BF)


def kernel(nblk, ngrp, chunk, sub, sat_hbm, ter_hbm, probes_hbm, row_ref, col_ref, trace_ref,
           mats, high, low, probes, slab, tiles, parts, gathered, traces, outgoing, incoming,
           mat_sem, probe_sem, slab_sem, slab_send, slab_recv, one_send, one_recv, two_send, two_recv,
           trace_send, trace_recv, mirror_send, mirror_recv):
    blk, grp = lax.axis_index("blk"), lax.axis_index("grp")
    rows, cols = sat_hbm.shape
    nprobe = probes_hbm.shape[0]
    nchunk = cols // chunk
    width = cols // ngrp
    nsub = width // sub
    total = nblk * ngrp
    me = blk * ngrp + grp
    ntile = tiles.shape[0]
    lanes = rows // 128
    stride = nblk // ntile
    barrier = pltpu.get_barrier_semaphore()
    row0 = pl.multiple_of(grp * rows, rows)

    slab_copy = pltpu.make_async_copy(probes_hbm.at[:, pl.ds(row0, rows)], slab, slab_sem)
    pl.when(blk == 0)(slab_copy.start)
    probe_copy = pltpu.make_async_copy(probes_hbm, probes, probe_sem)
    probe_copy.start()
    loads = []
    for c in range(nchunk):
        for m, hbm in enumerate((sat_hbm, ter_hbm)):
            cut = pl.ds(c * chunk, chunk)
            load = pltpu.make_async_copy(hbm.at[:, cut], mats.at[m, :, cut], mat_sem.at[c, m])
            load.start()
            loads.append(load)

    def other(j):
        d = lax.rem(me + j, total)
        return (d // ngrp, lax.rem(d, ngrp))

    def greet(j, carry):
        pl.semaphore_signal(barrier, inc=1, device_id=other(j), device_id_type=MESH)
        return carry

    lax.fori_loop(1, total, greet, 0)

    def slab_to(j):
        return pltpu.make_async_remote_copy(
            src_ref=slab, dst_ref=slab, send_sem=slab_send.at[j], recv_sem=slab_recv,
            device_id=(jnp.int32(j), grp), device_id_type=MESH)

    @pl.when(blk == 0)
    def _():
        pl.semaphore_wait(barrier, total - 1)
        slab_copy.wait()
        for j in range(nblk - 1, 0, -1):
            slab_to(j).start()

    probe_copy.wait()
    p_high, p_low = halves(probes[...])
    p_both = jnp.concatenate([p_high, p_low], axis=0)
    contract = (((1,), (1,)), ((), ()))
    strict = [jnp.zeros((nprobe, rows), F32)] * 2
    waited = -(-(ngrp * rows) // chunk)
    for load in loads[:2 * waited]:
        load.wait()
    row_id = lax.broadcasted_iota(jnp.int32, (rows, rows), 0)
    col_id = lax.broadcasted_iota(jnp.int32, (rows, rows), 1)

    for m in range(2):
        @pl.when(blk == 0)
        def _():
            def clear(j, carry):
                mats[m, :, pl.ds(pl.multiple_of(j * rows, rows), rows)] = jnp.zeros((rows, rows), F32)
                return carry

            lax.fori_loop(0, grp, clear, 0)
            block = mats[m, :, pl.ds(row0, rows)]
            diagonal = jnp.sum(jnp.where(row_id == col_id, block, 0.0), axis=0, keepdims=True)
            row_ref[m] = slab[...] * diagonal
            mats[m, :, pl.ds(row0, rows)] = jnp.where(col_id > row_id, block, 0.0)

        @pl.when(blk != 0)
        def _():
            row_ref[m] = jnp.zeros((nprobe, rows), F32)

    for c in range(nchunk):
        cut = pl.ds(c * chunk, chunk)
        for m in range(2):
            if c >= waited:
                loads[2 * c + m].wait()
            m_high, m_low = halves(mats[m, :, cut])
            high[m, :, cut] = m_high
            low[m, :, cut] = m_low
            both = lax.dot_general(p_both[:, c * chunk:(c + 1) * chunk], m_high, contract, preferred_element_type=F32)
            rest = lax.dot_general(p_high[:, c * chunk:(c + 1) * chunk], m_low, contract, preferred_element_type=F32)
            strict[m] = strict[m] + ((both[nprobe:] + rest) + both[:nprobe])

    @pl.when(blk != 0)
    def _():
        pl.semaphore_wait(barrier, total - 1)

    upper = [strict[m] + row_ref[m] for m in range(2)]
    whole = jnp.concatenate(upper, axis=0)
    for k in range(ntile):
        i, j = k // lanes, k % lanes
        tiles[k] = whole[8 * i:8 * i + 8, 128 * j:128 * j + 128]

    def one_to(k):
        return pltpu.make_async_remote_copy(
            src_ref=tiles.at[k], dst_ref=parts.at[blk], send_sem=one_send.at[k], recv_sem=one_recv,
            device_id=(jnp.int32(k * stride), grp), device_id_type=MESH)

    for k in range(ntile):
        @pl.when(blk == k * stride)
        def _():
            parts[k * stride] = tiles[k]

        @pl.when(blk != k * stride)
        def _():
            one_to(k).start()

    @pl.when(blk != 0)
    def _():
        pltpu.make_async_remote_copy(
            src_ref=slab, dst_ref=slab, send_sem=slab_send.at[0], recv_sem=slab_recv,
            device_id=(jnp.int32(0), grp), device_id_type=MESH).wait_recv()

    s = slab[...]
    s_high, s_low = halves(s)
    s_both = jnp.concatenate([s_high, s_low], axis=0)

    def mirror(m, start):
        cut = pl.ds(pl.multiple_of(start, sub), sub)
        both = jnp.dot(s_both, high[m, :, cut], preferred_element_type=F32)
        rest = jnp.dot(s_high, low[m, :, cut], preferred_element_type=F32)
        return (both[nprobe:] + rest) + both[:nprobe]

    def mirror_to(k, q):
        return pltpu.make_async_remote_copy(
            src_ref=outgoing.at[k - 1, q], dst_ref=incoming.at[k - 1, q],
            send_sem=mirror_send.at[k - 1, q], recv_sem=mirror_recv.at[k - 1, q],
            device_id=(blk, lax.rem(grp + k, ngrp)), device_id_type=MESH)

    def trace_to(j):
        return pltpu.make_async_remote_copy(
            src_ref=traces.at[me], dst_ref=traces.at[me], send_sem=trace_send, recv_sem=trace_recv,
            device_id=other(j), device_id_type=MESH)

    def send_trace():
        share = jnp.concatenate([s * (upper[m] + strict[m]) for m in range(2)], axis=0)
        share = jnp.sum(share, axis=1, keepdims=True)
        n = 2 * nprobe
        spot = lax.broadcasted_iota(jnp.int32, (n, 128), 0) == lax.broadcasted_iota(jnp.int32, (n, 128), 1)
        traces[me] = jnp.sum(jnp.where(spot, share, 0.0), axis=0, keepdims=True)

        def go(j, carry):
            trace_to(j).start()
            return carry

        lax.fori_loop(1, total, go, 0)

    for k in range(1, ngrp):
        base = lax.rem(grp + k, ngrp) * width
        for q in range(nsub):
            for m in range(2):
                outgoing[k - 1, q, m] = mirror(m, base + q * sub)
            mirror_to(k, q).start()
            if k == 1 and q == 0:
                send_trace()

    for q in range(nsub):
        for m in range(2):
            col_ref[m, :, q * sub:(q + 1) * sub] = mirror(m, grp * width + q * sub)

    def two_to(k, j):
        return pltpu.make_async_remote_copy(
            src_ref=gathered.at[k], dst_ref=gathered.at[k], send_sem=two_send.at[j], recv_sem=two_recv.at[k],
            device_id=(lax.rem(blk + j, nblk), grp), device_id_type=MESH)

    for k in range(ntile):
        @pl.when(blk == k * stride)
        def _():
            few = parts.at[pl.ds(0, nblk - 1)]
            pltpu.make_async_copy(few, few, one_recv).wait()
            got = parts[0]
            for b in range(1, nblk):
                got = got + parts[b]
            gathered[k] = got
            for j in range(1, nblk):
                two_to(k, j).start()

    for k in range(1, ngrp):
        for q in range(nsub):
            mirror_to(k, q).wait_recv()
            for m in range(2):
                cut = slice(q * sub, (q + 1) * sub)
                col_ref[m, :, cut] = col_ref[m, :, cut] + incoming[k - 1, q, m]

    most = traces.at[pl.ds(0, total - 1)]
    pltpu.make_async_copy(most, most, trace_recv).wait()
    line = jnp.sum(traces[...], axis=0)
    for m in range(2):
        trace_ref[m:m + 1, :] = line[:, m * nprobe:(m + 1) * nprobe]

    for k in range(ntile):
        @pl.when(blk != k * stride)
        def _():
            two_to(k, 1).wait_recv()

        i, j = k // lanes, k % lanes
        m, r = (8 * i) // nprobe, (8 * i) % nprobe
        row_ref[m, r:r + 8, 128 * j:128 * j + 128] = gathered[k]

    @pl.when(blk == 0)
    def _():
        for j in range(nblk - 1, 0, -1):
            slab_to(j).wait_send()

    for k in range(ntile):
        @pl.when(blk != k * stride)
        def _():
            one_to(k).wait_send()

        @pl.when(blk == k * stride)
        def _():
            for j in range(1, nblk):
                two_to(k, j).wait_send()

    for k in range(1, ngrp):
        for q in range(nsub):
            mirror_to(k, q).wait_send()
    pltpu.make_async_copy(most, most, trace_send).wait()


def solution(mesh):
    nblk, ngrp = mesh.shape["blk"], mesh.shape["grp"]

    def shards(matrix_sat, matrix_ter, probes):
        rows, cols = matrix_sat.shape
        nprobe = probes.shape[0]
        chunk = min(1024, cols)
        width = cols // ngrp
        sub = min(512, width)
        nsub = width // sub
        ntile = (2 * nprobe // 8) * (rows // 128)
        far = max(ngrp - 1, 1)
        dma = pltpu.SemaphoreType.DMA
        hbm = pl.BlockSpec(memory_space=pltpu.MemorySpace.HBM)
        vmem = pl.BlockSpec(memory_space=pltpu.MemorySpace.VMEM)
        return tuple(pl.pallas_call(
            functools.partial(kernel, nblk, ngrp, chunk, sub),
            out_shape=[
                jax.ShapeDtypeStruct((2, nprobe, rows), F32),
                jax.ShapeDtypeStruct((2, nprobe, width), F32),
                jax.ShapeDtypeStruct((2, nprobe), F32),
            ],
            in_specs=[hbm] * 3,
            out_specs=[vmem] * 3,
            scratch_shapes=[
                pltpu.VMEM((2, rows, cols), F32),
                pltpu.VMEM((2, rows, cols), BF),
                pltpu.VMEM((2, rows, cols), BF),
                pltpu.VMEM((nprobe, cols), F32),
                pltpu.VMEM((nprobe, rows), F32),
                pltpu.VMEM((ntile, 8, 128), F32),
                pltpu.VMEM((nblk, 8, 128), F32),
                pltpu.VMEM((ntile, 8, 128), F32),
                pltpu.VMEM((nblk * ngrp, 1, 128), F32),
                pltpu.VMEM((far, nsub, 2, nprobe, sub), F32),
                pltpu.VMEM((far, nsub, 2, nprobe, sub), F32),
                dma((cols // chunk, 2)),
                dma, dma,
                dma((nblk,)), dma,
                dma((ntile,)), dma,
                dma((nblk,)), dma((ntile,)),
                dma, dma,
                dma((far, nsub)), dma((far, nsub)),
            ],
            compiler_params=pltpu.CompilerParams(
                collective_id=0, has_side_effects=True, vmem_limit_bytes=48 * 1024 * 1024),
            name="trace_step",
        )(matrix_sat, matrix_ter, probes))

    in_specs = (P("grp", "blk"), P("grp", "blk"), P(None, "blk"))
    out_specs = (P(None, None, "grp"), P(None, None, ("blk", "grp")), P())
    return jax.shard_map(shards, mesh=mesh, in_specs=in_specs, out_specs=out_specs, check_vma=False)
```

```python
import functools

import jax
import jax.numpy as jnp
from jax import lax
from jax.experimental import pallas as pl
from jax.experimental.pallas import tpu as pltpu
from jax.sharding import PartitionSpec as P

MESH = pl.DeviceIdType.MESH
BF = jnp.bfloat16
F32 = jnp.float32


def halves(x):
    high = x.astype(BF)
    return high, (x - high.astype(F32)).astype(BF)


def kernel(nblk, ngrp, chunk, sub, sat_hbm, ter_hbm, probes_hbm, row_ref, col_ref, trace_ref,
           mats, high, low, probes, slab, tiles, parts, gathered, traces, finals, outgoing, incoming,
           mat_sem, probe_sem, slab_sem, slab_send, slab_recv, one_send, one_recv, two_send, two_recv,
           trace_send, trace_recv, final_send, final_recv, mirror_send, mirror_recv):
    blk, grp = lax.axis_index("blk"), lax.axis_index("grp")
    rows, cols = sat_hbm.shape
    nprobe = probes_hbm.shape[0]
    nchunk = cols // chunk
    width = cols // ngrp
    nsub = width // sub
    ntile = tiles.shape[0]
    lanes = rows // 128
    stride = nblk // ntile
    barrier = pltpu.get_barrier_semaphore()
    row0 = pl.multiple_of(grp * rows, rows)

    slab_copy = pltpu.make_async_copy(probes_hbm.at[:, pl.ds(row0, rows)], slab, slab_sem)
    pl.when(blk == 0)(slab_copy.start)
    probe_copy = pltpu.make_async_copy(probes_hbm, probes, probe_sem)
    probe_copy.start()
    loads = []
    for c in range(nchunk):
        for m, hbm in enumerate((sat_hbm, ter_hbm)):
            cut = pl.ds(c * chunk, chunk)
            load = pltpu.make_async_copy(hbm.at[:, cut], mats.at[m, :, cut], mat_sem.at[c, m])
            load.start()
            loads.append(load)

    def member(j):
        return (lax.rem(blk + j, nblk), grp)

    def peer(k):
        return (blk, lax.rem(grp + k, ngrp))

    friends = nblk - 1 + ngrp - 1
    for j in range(1, nblk):
        pl.semaphore_signal(barrier, inc=1, device_id=member(j), device_id_type=MESH)
    for k in range(1, ngrp):
        pl.semaphore_signal(barrier, inc=1, device_id=peer(k), device_id_type=MESH)

    def slab_to(j):
        return pltpu.make_async_remote_copy(
            src_ref=slab, dst_ref=slab, send_sem=slab_send.at[j], recv_sem=slab_recv,
            device_id=(jnp.int32(j), grp), device_id_type=MESH)

    pl.when(blk == 0)(slab_copy.wait)

    probe_copy.wait()
    p_high, p_low = halves(probes[...])
    p_both = jnp.concatenate([p_high, p_low], axis=0)
    contract = (((1,), (1,)), ((), ()))
    strict = [jnp.zeros((nprobe, rows), F32)] * 2
    waited = -(-(ngrp * rows) // chunk)
    for load in loads[:2 * waited]:
        load.wait()
    row_id = lax.broadcasted_iota(jnp.int32, (rows, rows), 0)
    col_id = lax.broadcasted_iota(jnp.int32, (rows, rows), 1)

    for m in range(2):
        @pl.when(blk == 0)
        def _():
            def clear(j, carry):
                mats[m, :, pl.ds(pl.multiple_of(j * rows, rows), rows)] = jnp.zeros((rows, rows), F32)
                return carry

            lax.fori_loop(0, grp, clear, 0)
            block = mats[m, :, pl.ds(row0, rows)]
            diagonal = jnp.sum(jnp.where(row_id == col_id, block, 0.0), axis=0, keepdims=True)
            row_ref[m] = slab[...] * diagonal
            mats[m, :, pl.ds(row0, rows)] = jnp.where(col_id > row_id, block, 0.0)

        @pl.when(blk != 0)
        def _():
            row_ref[m] = jnp.zeros((nprobe, rows), F32)

    for c in range(nchunk):
        cut = pl.ds(c * chunk, chunk)
        for m in range(2):
            if c >= waited:
                loads[2 * c + m].wait()
            m_high, m_low = halves(mats[m, :, cut])
            high[m, :, cut] = m_high
            low[m, :, cut] = m_low
            both = lax.dot_general(p_both[:, c * chunk:(c + 1) * chunk], m_high, contract, preferred_element_type=F32)
            rest = lax.dot_general(p_high[:, c * chunk:(c + 1) * chunk], m_low, contract, preferred_element_type=F32)
            strict[m] = strict[m] + ((both[nprobe:] + rest) + both[:nprobe])
        if c == max(nchunk - 2, 0):
            @pl.when(blk == 0)
            def _():
                pl.semaphore_wait(barrier, friends)
                for j in range(nblk - 1, 0, -1):
                    slab_to(j).start()

    @pl.when(blk != 0)
    def _():
        pl.semaphore_wait(barrier, friends)

    upper = [strict[m] + row_ref[m] for m in range(2)]
    whole = jnp.concatenate(upper, axis=0)
    for k in range(ntile):
        i, j = k // lanes, k % lanes
        tiles[k] = whole[8 * i:8 * i + 8, 128 * j:128 * j + 128]

    def one_to(k):
        return pltpu.make_async_remote_copy(
            src_ref=tiles.at[k], dst_ref=parts.at[blk], send_sem=one_send.at[k], recv_sem=one_recv,
            device_id=(jnp.int32(k * stride), grp), device_id_type=MESH)

    for k in range(ntile):
        @pl.when(blk == k * stride)
        def _():
            parts[k * stride] = tiles[k]

        @pl.when(blk != k * stride)
        def _():
            one_to(k).start()

    @pl.when(blk != 0)
    def _():
        pltpu.make_async_remote_copy(
            src_ref=slab, dst_ref=slab, send_sem=slab_send.at[0], recv_sem=slab_recv,
            device_id=(jnp.int32(0), grp), device_id_type=MESH).wait_recv()

    s = slab[...]
    s_high, s_low = halves(s)
    s_both = jnp.concatenate([s_high, s_low], axis=0)

    def mirror(m, start):
        cut = pl.ds(pl.multiple_of(start, sub), sub)
        both = jnp.dot(s_both, high[m, :, cut], preferred_element_type=F32)
        rest = jnp.dot(s_high, low[m, :, cut], preferred_element_type=F32)
        return (both[nprobe:] + rest) + both[:nprobe]

    def mirror_to(k, q):
        return pltpu.make_async_remote_copy(
            src_ref=outgoing.at[k - 1, q], dst_ref=incoming.at[k - 1, q],
            send_sem=mirror_send.at[k - 1, q], recv_sem=mirror_recv.at[k - 1, q],
            device_id=peer(k), device_id_type=MESH)

    def trace_to(j):
        return pltpu.make_async_remote_copy(
            src_ref=traces.at[blk], dst_ref=traces.at[blk], send_sem=trace_send.at[j], recv_sem=trace_recv,
            device_id=member(j), device_id_type=MESH)

    def send_trace():
        share = jnp.concatenate([s * (upper[m] + strict[m]) for m in range(2)], axis=0)
        share = jnp.sum(share, axis=1, keepdims=True)
        n = 2 * nprobe
        spot = lax.broadcasted_iota(jnp.int32, (n, 128), 0) == lax.broadcasted_iota(jnp.int32, (n, 128), 1)
        traces[blk] = jnp.sum(jnp.where(spot, share, 0.0), axis=0, keepdims=True)
        for j in range(1, nblk):
            trace_to(j).start()

    def final_to(k):
        return pltpu.make_async_remote_copy(
            src_ref=finals.at[grp], dst_ref=finals.at[grp], send_sem=final_send.at[k], recv_sem=final_recv.at[k],
            device_id=peer(k), device_id_type=MESH)

    for k in range(1, ngrp):
        base = lax.rem(grp + k, ngrp) * width
        for q in range(nsub):
            for m in range(2):
                outgoing[k - 1, q, m] = mirror(m, base + q * sub)
            mirror_to(k, q).start()
            if k == 1 and q == 0:
                send_trace()

    for q in range(nsub):
        for m in range(2):
            col_ref[m, :, q * sub:(q + 1) * sub] = mirror(m, grp * width + q * sub)

    def two_to(k, j):
        return pltpu.make_async_remote_copy(
            src_ref=gathered.at[k], dst_ref=gathered.at[k], send_sem=two_send.at[j], recv_sem=two_recv.at[k],
            device_id=member(j), device_id_type=MESH)

    for k in range(ntile):
        @pl.when(blk == k * stride)
        def _():
            few = parts.at[pl.ds(0, nblk - 1)]
            pltpu.make_async_copy(few, few, one_recv).wait()
            got = parts[0]
            for b in range(1, nblk):
                got = got + parts[b]
            gathered[k] = got
            for j in range(1, nblk):
                two_to(k, j).start()

    most = traces.at[pl.ds(0, nblk - 1)]
    pltpu.make_async_copy(most, most, trace_recv).wait()
    finals[grp] = jnp.sum(traces[...], axis=0)
    for k in range(1, ngrp):
        final_to(k).start()

    for k in range(1, ngrp):
        for q in range(nsub):
            mirror_to(k, q).wait_recv()
            for m in range(2):
                cut = slice(q * sub, (q + 1) * sub)
                col_ref[m, :, cut] = col_ref[m, :, cut] + incoming[k - 1, q, m]

    for k in range(1, ngrp):
        final_to(k).wait_recv()
    line = jnp.sum(finals[...], axis=0)
    for m in range(2):
        trace_ref[m:m + 1, :] = line[:, m * nprobe:(m + 1) * nprobe]

    for k in range(ntile):
        @pl.when(blk != k * stride)
        def _():
            two_to(k, 1).wait_recv()

        i, j = k // lanes, k % lanes
        m, r = (8 * i) // nprobe, (8 * i) % nprobe
        row_ref[m, r:r + 8, 128 * j:128 * j + 128] = gathered[k]

    @pl.when(blk == 0)
    def _():
        for j in range(nblk - 1, 0, -1):
            slab_to(j).wait_send()

    for k in range(ntile):
        @pl.when(blk != k * stride)
        def _():
            one_to(k).wait_send()

        @pl.when(blk == k * stride)
        def _():
            for j in range(1, nblk):
                two_to(k, j).wait_send()

    for k in range(1, ngrp):
        for q in range(nsub):
            mirror_to(k, q).wait_send()
    for j in range(1, nblk):
        trace_to(j).wait_send()
    for k in range(1, ngrp):
        final_to(k).wait_send()


def put_out(row_in, col_in, trace_in, row_out, col_out, trace_out, sem):
    pairs = ((col_in, col_out), (row_in, row_out), (trace_in, trace_out))
    copies = [pltpu.make_async_copy(a, b, sem.at[i]) for i, (a, b) in enumerate(pairs)]
    for copy in copies:
        copy.start()
    for copy in copies:
        copy.wait()


def solution(mesh):
    nblk, ngrp = mesh.shape["blk"], mesh.shape["grp"]

    def shards(matrix_sat, matrix_ter, probes):
        rows, cols = matrix_sat.shape
        nprobe = probes.shape[0]
        chunk = min(1024, cols)
        width = cols // ngrp
        sub = min(512, width)
        nsub = width // sub
        ntile = (2 * nprobe // 8) * (rows // 128)
        far = max(ngrp - 1, 1)
        dma = pltpu.SemaphoreType.DMA
        hbm = pl.BlockSpec(memory_space=pltpu.MemorySpace.HBM)
        vmem = pl.BlockSpec(memory_space=pltpu.MemorySpace.VMEM)
        parts = pl.pallas_call(
            functools.partial(kernel, nblk, ngrp, chunk, sub),
            out_shape=[
                jax.ShapeDtypeStruct((2, nprobe, rows), F32),
                jax.ShapeDtypeStruct((2, nprobe, width), F32),
                jax.ShapeDtypeStruct((2, nprobe), F32),
            ],
            in_specs=[hbm] * 3,
            out_specs=[vmem] * 3,
            scratch_shapes=[
                pltpu.VMEM((2, rows, cols), F32),
                pltpu.VMEM((2, rows, cols), BF),
                pltpu.VMEM((2, rows, cols), BF),
                pltpu.VMEM((nprobe, cols), F32),
                pltpu.VMEM((nprobe, rows), F32),
                pltpu.VMEM((ntile, 8, 128), F32),
                pltpu.VMEM((nblk, 8, 128), F32),
                pltpu.VMEM((ntile, 8, 128), F32),
                pltpu.VMEM((nblk, 1, 128), F32),
                pltpu.VMEM((ngrp, 1, 128), F32),
                pltpu.VMEM((far, nsub, 2, nprobe, sub), F32),
                pltpu.VMEM((far, nsub, 2, nprobe, sub), F32),
                dma((cols // chunk, 2)),
                dma, dma,
                dma((nblk,)), dma,
                dma((ntile,)), dma,
                dma((nblk,)), dma((ntile,)),
                dma((nblk,)), dma,
                dma((ngrp,)), dma((ngrp,)),
                dma((far, nsub)), dma((far, nsub)),
            ],
            compiler_params=pltpu.CompilerParams(
                collective_id=0, has_side_effects=True, vmem_limit_bytes=67043328),
            name="trace_step",
        )(matrix_sat, matrix_ter, probes)
        return tuple(pl.pallas_call(
            put_out,
            out_shape=[jax.ShapeDtypeStruct(part.shape, F32) for part in parts],
            in_specs=[vmem] * 3,
            out_specs=[hbm] * 3,
            scratch_shapes=[dma((3,))],
            name="put_out",
        )(*parts))

    in_specs = (P("grp", "blk"), P("grp", "blk"), P(None, "blk"))
    out_specs = (P(None, None, "grp"), P(None, None, ("blk", "grp")), P())
    return jax.shard_map(shards, mesh=mesh, in_specs=in_specs, out_specs=out_specs, check_vma=False)
```
